32 devices in a mesh: dp: 4 (over y, x), seq: 4 (over z), tensor: 2 (over core).
Axes of the slice: x: 2, y: 2, z: 4, core: 2. Of those that a mesh axis runs over, the one named last changes fastest.
Arguments:
- tokens: bfloat16 [8, 1024, 2048], P('dp', 'seq'), may hold values from -6 to 6
- out_grad: bfloat16 [8, 1024, 2048], P('dp', 'seq'), may hold values from -6 to 6
- lengths: int32 [8], P('dp'), may hold values from 256 to 1024, as said below
- master: float32 [2048, 24576], P(('dp', 'seq'), 'tensor')
- moment_m: float32 [2048, 24576], P(('dp', 'seq'), 'tensor')
- moment_v: float32 [2048, 24576], P(('dp', 'seq'), 'tensor'), may hold values from 2.21184 to 35.2256
- gains: float32 [4352], P(('dp', 'seq')), may hold values from 0.5 to 2
- gains_m: float32 [4352], P(('dp', 'seq')), may hold values from -48 to 48
- gains_v: float32 [4352], P(('dp', 'seq')), may hold values from 24.576 to 2457.6
Outputs:
- block_out: bfloat16 [8, 1024, 2048], P('dp', 'seq')
- input_grad: float32 [8, 1024, 2048], P('dp', 'seq')
- new_master: float32 [2048, 24576], P(('dp', 'seq'), 'tensor')
- new_m: float32 [2048, 24576], P(('dp', 'seq'), 'tensor')
- new_v: float32 [2048, 24576], P(('dp', 'seq'), 'tensor')
- new_copy: bfloat16 [2048, 24576], P(('dp', 'seq'), 'tensor')
- gains_new: float32 [4352], P(('dp', 'seq'))
- gains_first: float32 [4352], P(('dp', 'seq'))
- gains_second: float32 [4352], P(('dp', 'seq'))
- norms: float32 [2, 11], replicated
The draws below stay inside these ranges and needn't reach their ends.
Inputs may be any that keep to these rules, and one draw needn't show every extreme that they name: Each sequence holds lengths[b] real tokens at its first slots; one sequence has all 1024 slots real and another exactly 256.
All inputs are finite; a program needn't handle non-finite values.
Results may differ from the reference program's by a relative error of at most 0.018.
The reference program's roundings to bfloat16 on the way count: a program that leaves them out, or rounds other values in their place, can miss the bound.
Values may be sent and summed in bfloat16 or wider, within the bound.
A program may use at most 448 MiB of HBM per device.

```python
import math
import jax
import jax.numpy as jnp
from jax import lax

D = 2048
HQ = 16
KVH = 8
HD = 128
FF = 6144
LEN = 1024
BATCH = 8
ALLTOK = 8192
NG = 4352
WTOT = 24576
WPART = 12288
QW = 1024
KW = 512
FW = 3072
N_TENSOR = 2


def rise_rows(row_count, steepness):
    return jnp.power(steepness, jnp.arange(row_count, dtype=jnp.float32) / row_count)


def column_scales():
    col_idx = jnp.arange(WTOT, dtype=jnp.int32) % WPART
    out_start = QW + 2 * KW
    out_stop = 2 * QW + 2 * KW
    down_start = 2 * QW + 2 * KW + 2 * FW
    in_scale = jnp.full((WTOT,), D ** (-0.5), jnp.float32)
    scales = jnp.where((col_idx >= out_start) & (col_idx < out_stop), 4.0 * (HQ * HD) ** (-0.5), in_scale)
    return jnp.where(col_idx >= down_start, FF ** (-0.5), scales)


def draw_lengths(key, part):
    first_key, second_key, third_key = jax.random.split(key, 3)
    drawn = jax.random.randint(first_key, (BATCH,), LEN // 4, LEN + 1)
    top_at = jax.random.randint(second_key, (), 0, BATCH)
    least_at = (top_at + 1 + jax.random.randint(third_key, (), 0, BATCH - 1)) % BATCH
    seq_idx = jnp.arange(BATCH)
    drawn = jnp.where(seq_idx == top_at, LEN, drawn)
    drawn = jnp.where(seq_idx == least_at, LEN // 4, drawn)
    return drawn.astype(jnp.int32)


def draw_master(key, part):
    raw_vals = jax.random.normal(key, (D, WTOT), jnp.float32)
    row_scale = rise_rows(D, 3.0) / 1.9
    return raw_vals * row_scale[:, None] * column_scales()[None, :]


def draw_moment_m(key, part):
    size_scale = 0.026 * ALLTOK ** 0.5
    raw_vals = jax.random.normal(key, (D, WTOT), jnp.float32)
    row_scale = rise_rows(D, 3.0) / 1.9
    return raw_vals * row_scale[:, None] * size_scale


def block_levels(rng, extent, pieces, least, top_value):
    factor_of = 1.0
    for dim, blocks in pieces:
        heights = jax.random.uniform(jax.random.fold_in(jax.random.fold_in(rng, 6), dim), (blocks,), jnp.float32, least / len(pieces), top_value / len(pieces))
        factor_of = factor_of * jnp.repeat(jnp.exp(heights), extent[dim] // blocks).reshape((-1,) + (1,) * (len(extent) - 1 - dim))
    return factor_of


def bell_draw(stream_key, dims, width, most, pieces=(), kind=jnp.bfloat16):
    entries = jax.random.normal(stream_key, dims, jnp.float32) * width
    if len(pieces) > 0:
        entries = block_levels(stream_key, dims, pieces, -0.22, 0.18) * entries
    return jnp.clip(entries, min=-most, max=most).astype(kind)


def setup_inputs(seed: int = 0) -> dict:
    keys = jax.random.split(jax.random.key(seed), 10)
    return {
        "tokens": bell_draw(keys[0], (BATCH, LEN, D), 1.0, 6.0, ((0, 4), (1, 4))),
        "out_grad": bell_draw(keys[1], (BATCH, LEN, D), 1.0, 6.0, ((0, 4), (1, 4))),
        "lengths": draw_lengths(jax.random.fold_in(keys[9], 71), 0),
        "master": draw_master(jax.random.fold_in(keys[9], 71), 0),
        "moment_m": draw_moment_m(jax.random.fold_in(keys[9], 71), 0),
        "moment_v": jnp.clip(jnp.exp(math.log(35.2256) - 2.7679484 * jax.random.uniform(keys[5], (D, WTOT), jnp.float32) ** block_levels(keys[5], (D, WTOT), ((0, 16), (1, 2)), -0.2, 0.2)), 2.21184, 35.2256),
        "gains": jnp.clip(0.5 + 1.5 * jax.random.uniform(keys[6], (NG,), jnp.float32) ** block_levels(keys[6], (NG,), ((0, 16),), -0.2, 0.2), 0.5, 2.0),
        "gains_m": bell_draw(keys[7], (NG,), (0.085 * ALLTOK ** 0.5), 48.0, ((0, 16),), jnp.float32),
        "gains_v": jnp.clip(jnp.exp(math.log(2457.6) - 4.6051702 * jax.random.uniform(keys[8], (NG,), jnp.float32) ** block_levels(keys[8], (NG,), ((0, 16),), -0.2, 0.2)), 24.576, 2457.6),
    }


EPS_NORM = 1e-06
ROPE_BASE = 1000000.0
BETA_ONE = 0.9
BETA_TWO = 0.99
ADAM_EPS = 1e-06
WEIGHT_DECAY = 0.01
LEARN_RATE = 0.3
MASKED = -1e+30
HIGH_PREC = lax.Precision.HIGHEST

@jax.custom_vjp
def low(v):
    return lax.optimization_barrier(v.astype(jnp.bfloat16)).astype(jnp.float32)

@jax.custom_vjp
def low_back(v):
    return v

def low_keep(v):
    return (low(v), None)

def low_pass(kept, grad):
    return (grad,)

def back_keep(v):
    return (v, None)

def back_low(kept, grad):
    return (low(grad),)
low.defvjp(low_keep, low_pass)
low_back.defvjp(back_keep, back_low)

def mat_mul(left_val, right_val):
    return jnp.dot(left_val, right_val, precision=HIGH_PREC, preferred_element_type=jnp.float32)

def rms_of(values):
    return lax.rsqrt(lax.optimization_barrier(jnp.mean(values * values, axis=-1, keepdims=True)) + EPS_NORM)

def turn_half(values):
    half_dim = values.shape[-1] // 2
    return jnp.concatenate([-values[..., half_dim:], values[..., :half_dim]], axis=-1)

def rope_tables(positions):
    half_dim = HD // 2
    freq_idx = jnp.arange(half_dim, dtype=jnp.float32)
    inv_freq = jnp.power(ROPE_BASE, -2.0 * freq_idx / HD)
    angles = positions.astype(jnp.float32)[:, None] * inv_freq[None, :]
    angles = jnp.concatenate([angles, angles], axis=-1)
    return (jnp.cos(angles)[:, None, :], jnp.sin(angles)[:, None, :])

def offsets():
    off_k = QW
    off_v = off_k + KW
    output_offset = off_v + KW
    gate_offset = output_offset + QW
    off_u = gate_offset + FW
    down_offset = off_u + FW
    return (off_k, off_v, output_offset, gate_offset, off_u, down_offset)

def columns(flat_w, start_col, stop_col):
    split_w = flat_w.reshape(D, N_TENSOR, WPART)[:, :, start_col:stop_col]
    return split_w.reshape(D, N_TENSOR * (stop_col - start_col))

def attend(q_rot, k_rot, v_low, seq_len):
    q_block = min(512, LEN)
    block_count = LEN // q_block
    group_size = HQ // KVH
    key_pos = jnp.arange(LEN, dtype=jnp.int32)
    q_blocks = q_rot.reshape(block_count, q_block, KVH, group_size, HD)
    starts = jnp.arange(block_count, dtype=jnp.int32) * q_block

    def one_block(block_args):
        q_part, first_row = block_args
        raw_scores = jnp.einsum('bkgd,jkd->kgbj', q_part, k_rot, precision=HIGH_PREC) * HD ** (-0.5)
        scores = low_back(raw_scores)
        q_pos = first_row + jnp.arange(q_block, dtype=jnp.int32)
        allowed = (key_pos[None, :] <= q_pos[:, None]) & (key_pos[None, :] < seq_len)
        scores = jnp.where(allowed, scores, MASKED)
        probs = low(jax.nn.softmax(scores, axis=-1))
        mixed = jnp.einsum('kgbj,jkd->bkgd', probs, v_low, precision=HIGH_PREC)
        return mixed.reshape(q_block, HQ * HD)
    return lax.map(jax.checkpoint(one_block), (q_blocks, starts)).reshape(LEN, HQ * HD)

def forward(x_in, flat_w, gain_all, seq_len):
    off_k, off_v, output_offset, gate_offset, off_u, down_offset = offsets()
    gain_one = gain_all[:D]
    gain_two = gain_all[D:2 * D]
    gain_q = gain_all[2 * D:2 * D + HD]
    gain_k = gain_all[2 * D + HD:]
    first_activation = low(x_in * rms_of(x_in) * gain_one)
    q_raw = low_back(mat_mul(first_activation, columns(flat_w, 0, off_k))).reshape(LEN, HQ, HD)
    k_raw = low_back(mat_mul(first_activation, columns(flat_w, off_k, off_v))).reshape(LEN, KVH, HD)
    v_low = low(low_back(mat_mul(first_activation, columns(flat_w, off_v, output_offset)))).reshape(LEN, KVH, HD)
    cos_t, sin_t = rope_tables(jnp.arange(LEN, dtype=jnp.int32))
    q_unit = q_raw * rms_of(q_raw) * gain_q
    q_rot = low(q_unit * cos_t + turn_half(q_unit) * sin_t)
    k_unit = k_raw * rms_of(k_raw) * gain_k
    k_rot = low(k_unit * cos_t + turn_half(k_unit) * sin_t)
    attn_mix = attend(q_rot, k_rot, v_low, seq_len)
    attention_reduced = low(low_back(attn_mix))
    resid_mid = x_in + low_back(mat_mul(attention_reduced, columns(flat_w, output_offset, gate_offset).T))
    second_activation = low(resid_mid * rms_of(resid_mid) * gain_two)
    gate_val = low_back(mat_mul(second_activation, columns(flat_w, gate_offset, off_u)))
    up_val = low_back(mat_mul(second_activation, columns(flat_w, off_u, down_offset)))
    hidden_reduced = low(jax.nn.silu(gate_val) * up_val)
    return resid_mid + low_back(mat_mul(hidden_reduced, columns(flat_w, down_offset, WPART).T))

def part_sums(values, seg_ids, seg_count):
    collapsed = lax.optimization_barrier(jnp.sum(values.reshape(-1, seg_ids.shape[0]), axis=0))
    return jax.ops.segment_sum(collapsed, seg_ids, seg_count)

def lamb_step(weight_old, grad_new, first_old, second_old, seg_ids, seg_count):
    first_new = BETA_ONE * first_old + (1.0 - BETA_ONE) * grad_new
    second_new = BETA_TWO * second_old + (1.0 - BETA_TWO) * grad_new * grad_new
    update = first_new / (jnp.sqrt(second_new) + ADAM_EPS) + WEIGHT_DECAY * weight_old
    weight_norm = jnp.sqrt(part_sums(weight_old * weight_old, seg_ids, seg_count))
    update_norm = jnp.sqrt(part_sums(update * update, seg_ids, seg_count))
    trust = weight_norm / (update_norm + ADAM_EPS)
    weight_new = weight_old - LEARN_RATE * trust[seg_ids] * update
    return (weight_new, first_new, second_new, weight_norm, update_norm)

def reference(tokens, out_grad, lengths, master, moment_m, moment_v, gains, gains_m, gains_v):
    copy_w = master.astype(jnp.bfloat16).astype(jnp.float32)
    copy_g = gains.astype(jnp.bfloat16).astype(jnp.float32)
    slot_idx = jnp.arange(LEN, dtype=jnp.int32)

    def one_seq(carry, item):
        acc_w, acc_g = carry
        seq_tokens, seq_grad, seq_len = item
        x_in = seq_tokens.astype(jnp.float32)
        result, pull_back = jax.vjp(lambda a_in, b_in, c_in: forward(a_in, b_in, c_in, seq_len), x_in, copy_w, copy_g)
        valid = (slot_idx < seq_len)[:, None]
        grad_x, grad_w, grad_g = pull_back(jnp.where(valid, seq_grad.astype(jnp.float32), 0.0))
        return ((acc_w + grad_w, acc_g + grad_g), (result.astype(jnp.bfloat16), grad_x))
    start_acc = (jnp.zeros((D, WTOT), jnp.float32), jnp.zeros((NG,), jnp.float32))
    (grad_w, grad_g), (block_out, input_grad) = lax.scan(one_seq, start_acc, (tokens, out_grad, lengths))
    col_idx = jnp.arange(WTOT, dtype=jnp.int32) % WPART
    seg_w = jnp.zeros((WTOT,), jnp.int32)
    for edge_val in offsets():
        seg_w = seg_w + (col_idx >= edge_val).astype(jnp.int32)
    gain_idx = jnp.arange(NG, dtype=jnp.int32)
    seg_g = jnp.zeros((NG,), jnp.int32)
    for edge_val in (D, 2 * D, 2 * D + HD):
        seg_g = seg_g + (gain_idx >= edge_val).astype(jnp.int32)
    new_w, first_w, second_w, wnorm_w, unorm_w = lamb_step(master, grad_w, moment_m, moment_v, seg_w, 7)
    new_g, first_g, second_g, wnorm_g, unorm_g = lamb_step(gains, grad_g, gains_m, gains_v, seg_g, 4)
    norms = jnp.stack([jnp.concatenate([wnorm_w, wnorm_g]), jnp.concatenate([unorm_w, unorm_g])])
    return (block_out, input_grad, new_w, first_w, second_w, new_w.astype(jnp.bfloat16), new_g, first_g, second_g, norms)
```

```python
import functools

import jax
import jax.numpy as jnp
from jax import lax
from jax.experimental import pallas as pl
from jax.experimental.pallas import tpu as pltpu
from jax.sharding import PartitionSpec as P

D = 2048
HQ = 16
KVH = 8
HD = 128
FF = 6144


EPS_NORM = 1e-06
ROPE_BASE = 1000000.0
BETA_ONE = 0.9
BETA_TWO = 0.99
ADAM_EPS = 1e-06
WEIGHT_DECAY = 0.01
LEARN_RATE = 0.3
MASKED = -1e30
SCALE = HD ** (-0.5)
PARTS = 11


F32 = jnp.float32
BF16 = jnp.bfloat16


def rms_of(values):
    return lax.rsqrt(jnp.mean(values * values, axis=-1, keepdims=True) + EPS_NORM)


def rms_back(grad_unit, unit_vals, scale_vals):
    return scale_vals * (
        grad_unit - unit_vals * jnp.mean(grad_unit * unit_vals, axis=-1, keepdims=True)
    )


def turn_half(values):
    half_dim = values.shape[-1] // 2
    return jnp.concatenate([-values[..., half_dim:], values[..., :half_dim]], axis=-1)


def turn_back(values):
    half_dim = values.shape[-1] // 2
    return jnp.concatenate([values[..., half_dim:], -values[..., :half_dim]], axis=-1)


def rope_tables(positions):
    half_dim = HD // 2
    freq_idx = jnp.arange(half_dim, dtype=F32)
    inv_freq = jnp.power(ROPE_BASE, -2.0 * freq_idx / HD)
    angles = positions.astype(F32)[:, None] * inv_freq[None, :]
    angles = jnp.concatenate([angles, angles], axis=-1)
    return (jnp.cos(angles), jnp.sin(angles))


def swap(values, axis, bit):
    size = lax.axis_size(axis)
    return lax.ppermute(values, axis, [(i, i ^ bit) for i in range(size)])


def swap_x(values):
    return swap(values, "dp", 1)


def swap_y(values):
    return swap(values, "dp", 2)


def swap_core(values):
    return swap(values, "tensor", 1)


def group_gather(block):
    rows = block.shape[0]
    half = rows // 2
    one, two = block[:half], block[half:]
    one_x, two_y = swap_x(one), swap_y(two)
    one_y = swap_y(jnp.stack([one, one_x]))
    two_x = swap_x(jnp.stack([two, two_y]))
    mine = jnp.concatenate(
        [one, two, one_x, two_x[0], one_y[0], two_y, one_y[1], two_x[1]], axis=0
    )
    other = swap_core(mine)
    return jnp.concatenate([mine, other], axis=0)


def group_scatter(partial_sums, rows):
    half = rows // 2
    split = partial_sums.reshape(2, 4, rows, partial_sums.shape[-1])
    other = swap_core(split[1])
    total = split[0].astype(F32) + other.astype(F32)
    low = total.astype(BF16)
    one_x = swap_x(jnp.stack([low[1, :half], low[3, :half]]))
    two_y = swap_y(jnp.stack([low[2, half:], low[3, half:]]))
    one_own = total[0, :half] + one_x[0].astype(F32)
    one_fwd = total[2, :half] + one_x[1].astype(F32)
    two_own = total[0, half:] + two_y[0].astype(F32)
    two_fwd = total[1, half:] + two_y[1].astype(F32)
    one_y = swap_y(one_fwd.astype(BF16))
    two_x = swap_x(two_fwd.astype(BF16))
    return jnp.concatenate(
        [one_own + one_y.astype(F32), two_own + two_x.astype(F32)], axis=0
    )


def softmax_rows(q_head, keys, allowed):
    scores = (
        lax.dot_general(q_head, keys, (((1,), (1,)), ((), ())), preferred_element_type=F32) * SCALE
    )
    scores = jnp.where(allowed, scores, MASKED)
    top = jnp.max(scores, axis=-1, keepdims=True)
    weights = jnp.exp(scores - top)
    return weights / jnp.sum(weights, axis=-1, keepdims=True)


def allowed_keys(info_ref, q_len, blocks):
    shape = (q_len, blocks * q_len)
    row = lax.broadcasted_iota(jnp.int32, shape, 0)
    col = lax.broadcasted_iota(jnp.int32, shape, 1)
    place = info_ref[0]
    slot = col // q_len
    key_pos = (place - slot) * q_len + (col - slot * q_len)
    q_pos = place * q_len + row
    length = info_ref[1 + pl.program_id(0)]
    return (key_pos >= 0) & (key_pos <= q_pos) & (key_pos < length)


def attend_kernel(info_ref, q_ref, *refs, q_len, blocks):
    kv_refs, out_ref = refs[:blocks], refs[blocks]
    keys = jnp.concatenate([r[:, :HD] for r in kv_refs], axis=0)
    vals = jnp.concatenate([r[:, HD:] for r in kv_refs], axis=0)
    allowed = allowed_keys(info_ref, q_len, blocks)
    heads = q_ref.shape[-1] // HD
    for h in range(heads):
        cols = slice(h * HD, (h + 1) * HD)
        probs = softmax_rows(q_ref[:, cols], keys, allowed).astype(BF16)
        out_ref[:, cols] = jnp.dot(probs, vals, preferred_element_type=F32).astype(BF16)


def attend_back_kernel(info_ref, q_ref, do_ref, *refs, q_len, blocks):
    kv_refs = refs[:blocks]
    dq_ref = refs[blocks]
    dkv_refs = refs[blocks + 1 :]
    keys = jnp.concatenate([r[:, :HD] for r in kv_refs], axis=0)
    vals = jnp.concatenate([r[:, HD:] for r in kv_refs], axis=0)
    allowed = allowed_keys(info_ref, q_len, blocks)
    heads = q_ref.shape[-1] // HD
    key_grad = jnp.zeros((blocks * q_len, HD), F32)
    val_grad = jnp.zeros((blocks * q_len, HD), F32)
    for h in range(heads):
        cols = slice(h * HD, (h + 1) * HD)
        q_head, do_head = q_ref[:, cols], do_ref[:, cols]
        probs = softmax_rows(q_head, keys, allowed)
        grad_probs = lax.dot_general(
            do_head, vals, (((1,), (1,)), ((), ())), preferred_element_type=F32
        )
        delta = jnp.sum(probs * grad_probs, axis=-1, keepdims=True)
        grad_scores = (probs * (grad_probs - delta)).astype(BF16)
        dq_ref[:, cols] = jnp.dot(grad_scores, keys, preferred_element_type=F32) * SCALE
        key_grad = key_grad + lax.dot_general(
            grad_scores, q_head, (((0,), (0,)), ((), ())), preferred_element_type=F32
        )
        val_grad = val_grad + lax.dot_general(
            probs.astype(BF16), do_head, (((0,), (0,)), ((), ())), preferred_element_type=F32
        )
    for s in range(blocks):
        rows = slice(s * q_len, (s + 1) * q_len)
        dkv_refs[s][:, :HD] = (key_grad[rows] * SCALE).astype(dkv_refs[s].dtype)
        dkv_refs[s][:, HD:] = val_grad[rows].astype(dkv_refs[s].dtype)


def row_spec(q_len, width):
    return pl.BlockSpec((q_len, width), lambda i, info: (i, 0))


def attend(info, q_low, kv_blocks, q_len):
    count, width = q_low.shape[0] // q_len, q_low.shape[1]
    blocks = len(kv_blocks)
    flops = 4 * q_low.size * q_len * blocks
    return pl.pallas_call(
        functools.partial(attend_kernel, q_len=q_len, blocks=blocks),
        out_shape=jax.ShapeDtypeStruct(q_low.shape, BF16),
        grid_spec=pltpu.PrefetchScalarGridSpec(
            num_scalar_prefetch=1,
            grid=(count,),
            in_specs=[row_spec(q_len, width)] + [row_spec(q_len, 2 * HD)] * blocks,
            out_specs=row_spec(q_len, width),
        ),
        cost_estimate=pl.CostEstimate(
            flops=flops, bytes_accessed=12 * q_low.size, transcendentals=0
        ),
        name="attend",
    )(info, q_low, *kv_blocks)


def attend_back(info, q_low, do_low, kv_blocks, q_len):
    count, width = q_low.shape[0] // q_len, q_low.shape[1]
    blocks = len(kv_blocks)
    flops = 10 * q_low.size * q_len * blocks
    return pl.pallas_call(
        functools.partial(attend_back_kernel, q_len=q_len, blocks=blocks),
        out_shape=[jax.ShapeDtypeStruct(q_low.shape, F32)]
        + [jax.ShapeDtypeStruct(kv_blocks[0].shape, BF16)] * blocks,
        grid_spec=pltpu.PrefetchScalarGridSpec(
            num_scalar_prefetch=1,
            grid=(count,),
            in_specs=[row_spec(q_len, width)] * 2 + [row_spec(q_len, 2 * HD)] * blocks,
            out_specs=[row_spec(q_len, width)] + [row_spec(q_len, 2 * HD)] * blocks,
        ),
        cost_estimate=pl.CostEstimate(
            flops=flops, bytes_accessed=20 * q_low.size, transcendentals=0
        ),
        name="attend_back",
    )(info, q_low, do_low, *kv_blocks)


def adam_part(weight_old, grad_new, first_old, second_old):
    first_new = BETA_ONE * first_old + (1.0 - BETA_ONE) * grad_new
    second_new = BETA_TWO * second_old + (1.0 - BETA_TWO) * grad_new * grad_new
    update = first_new / (jnp.sqrt(second_new) + ADAM_EPS) + WEIGHT_DECAY * weight_old
    return (first_new, second_new, update)


def product(left, right, kind=F32):
    return jnp.dot(left, right, preferred_element_type=F32).astype(kind)


def product_wide(left, right, kind=F32):
    return lax.dot_general(
        left, right, (((1,), (1,)), ((), ())), preferred_element_type=F32
    ).astype(kind)


def product_tokens(left, right, kind=F32):
    return lax.dot_general(
        left, right, (((0,), (0,)), ((), ())), preferred_element_type=F32
    ).astype(kind)


def per_device(tokens, out_grad, lengths, master, moment_m, moment_v, gains, gains_m, gains_v):
    seq_count, q_len = (tokens.shape[0], tokens.shape[1])
    dp_size = lax.axis_size("dp")
    tensor_size = lax.axis_size("tensor")
    seq_size = lax.axis_size("seq")
    assert dp_size == 4 and tensor_size == 2 and seq_count == 2
    group = dp_size * tensor_size
    dp_at, seq_at, core_at = (lax.axis_index(a) for a in ("dp", "seq", "tensor"))
    rows = master.shape[0]
    q_cols, k_cols, f_cols = HQ * HD // group, KVH * HD // group, FF // group
    assert k_cols == HD
    widths = (q_cols, k_cols, k_cols, q_cols, f_cols, f_cols, f_cols)
    wide = tuple(dp_size * w for w in widths)
    starts = [0]
    for w in wide:
        starts.append(starts[-1] + w)

    def mix(values):
        split = values.reshape(values.shape[:-1] + (dp_size, seq_size, rows))
        return jnp.swapaxes(split, -3, -2).reshape(values.shape)

    def unmix(values):
        split = values.reshape(values.shape[:-1] + (seq_size, dp_size, rows))
        return jnp.swapaxes(split, -3, -2).reshape(values.shape)

    gain_len = gains.shape[0]
    g_full = lax.all_gather(gains.astype(BF16), ("dp", "seq"), axis=0, tiled=True)
    gain_f = g_full.astype(F32)
    gain_one = mix(gain_f[:D])
    gain_two = mix(gain_f[D : 2 * D])
    gain_q = gain_f[2 * D : 2 * D + HD]
    gain_k = gain_f[2 * D + HD :]

    def weights_of(mats):
        def quarter(r):
            return jnp.concatenate(
                [
                    lax.dynamic_slice_in_dim(
                        master, starts[m] + (dp_at ^ r) * widths[m], widths[m], 1
                    )
                    for m in mats
                ],
                axis=1,
            ).astype(BF16)

        parts = [quarter(r) for r in range(dp_size)]
        got = jnp.stack(
            [parts[0]] + [swap(parts[r], "dp", r) for r in range(1, dp_size)]
        )
        placed = jnp.stack([
            lax.dynamic_index_in_dim(got, dp_at ^ d, 0, keepdims=False) for d in range(dp_size)
        ])
        block = placed.reshape(dp_size * rows, -1)
        return lax.all_gather(block, "seq", axis=0, tiled=True)

    def grads_home(grad):
        mine = lax.psum_scatter(grad, "seq", scatter_dimension=0, tiled=True)
        split = mine.reshape(dp_size, rows, -1)
        sent = [
            lax.dynamic_index_in_dim(split, dp_at ^ r, 0, keepdims=False) for r in range(dp_size)
        ]
        got = jnp.stack([sent[0]] + [swap(sent[r], "dp", r) for r in range(1, dp_size)])
        return [
            lax.dynamic_index_in_dim(got, dp_at ^ d, 0, keepdims=False) for d in range(dp_size)
        ]

    w_qkv = weights_of((0, 1, 2))
    w_out = weights_of((3,))
    w_gu = weights_of((4, 5))
    w_down = weights_of((6,))

    pair = jnp.stack([
        lax.dynamic_index_in_dim(lengths, core_at, 0, keepdims=False),
        lax.dynamic_index_in_dim(lengths, 1 - core_at, 0, keepdims=False),
    ])[:, None]
    pair = jnp.concatenate([pair, swap_x(pair)], axis=1)
    pair = jnp.concatenate([pair, swap_y(pair)], axis=1)
    info = jnp.concatenate([seq_at[None].astype(jnp.int32), pair.reshape(-1)])

    in_f = mix(lax.dynamic_index_in_dim(tokens, core_at, 0, keepdims=False)).astype(F32)
    scale_one = rms_of(in_f)
    unit_one = in_f * scale_one
    act_one = group_gather((unit_one * gain_one).astype(BF16))
    q_pos = seq_at * q_len + jnp.arange(q_len, dtype=jnp.int32)
    my_length = lax.dynamic_index_in_dim(lengths, core_at, 0, keepdims=False)
    grad_in = mix(lax.dynamic_index_in_dim(out_grad, core_at, 0, keepdims=False)).astype(F32)
    grad_out_f = jnp.where((q_pos < my_length)[:, None], grad_in, 0.0)
    grad_out_all = group_gather(grad_out_f.astype(BF16))

    qkv = product(act_one, w_qkv)
    cos_t, sin_t = rope_tables(q_pos)
    cos_t = cos_t[None, :, None, :]
    sin_t = sin_t[None, :, None, :]
    q_raw = qkv[:, :q_cols].reshape(group, q_len, q_cols // HD, HD)
    k_raw = qkv[:, q_cols : q_cols + k_cols].reshape(group, q_len, 1, HD)
    v_low = qkv[:, q_cols + k_cols :].astype(BF16)
    k_scale = rms_of(k_raw)
    k_unit = k_raw * k_scale * gain_k
    k_low = (k_unit * cos_t + turn_half(k_unit) * sin_t).astype(BF16)
    kv_low = jnp.concatenate([k_low.reshape(-1, HD), v_low], axis=1)
    kv_blocks = [kv_low]
    ahead = [(i, i + 1) for i in range(seq_size - 1)]
    back = [(i + 1, i) for i in range(seq_size - 1)]
    for _ in range(seq_size - 1):
        kv_blocks.append(lax.ppermute(kv_blocks[-1], "seq", ahead))
    q_scale = rms_of(q_raw)
    q_unit = q_raw * q_scale * gain_q
    q_low = (q_unit * cos_t + turn_half(q_unit) * sin_t).astype(BF16).reshape(-1, q_cols)

    mixed = attend(info, q_low, kv_blocks, q_len)
    attn_part = product_wide(mixed, w_out, BF16)
    resid_mid = in_f + group_scatter(attn_part, q_len)
    scale_two = rms_of(resid_mid)
    unit_two = resid_mid * scale_two
    act_two = group_gather((unit_two * gain_two).astype(BF16))
    gate_up = product(act_two, w_gu)
    gate_val, up_val = gate_up[:, :f_cols], gate_up[:, f_cols:]
    gate_sig = jax.nn.sigmoid(gate_val)
    silu_val = gate_val * gate_sig
    hidden = (silu_val * up_val).astype(BF16)
    grad_hidden = product(grad_out_all, w_down)
    grad_gate = (grad_hidden * up_val * gate_sig * (1.0 + gate_val * (1.0 - gate_sig))).astype(BF16)
    grad_up = (grad_hidden * silu_val).astype(BF16)
    grad_gu = jnp.concatenate([grad_gate, grad_up], axis=1)
    grad_act_two = group_scatter(product_wide(grad_gu, w_gu, BF16), q_len)

    block_out = resid_mid + group_scatter(product_wide(hidden, w_down, BF16), q_len)
    home_down = grads_home(product_tokens(grad_out_all, hidden, BF16))
    home_gu = grads_home(product_tokens(act_two, grad_gu, BF16))

    gain_two_part = jnp.sum(grad_act_two * unit_two, axis=0)
    resid_grad = grad_out_f + rms_back(grad_act_two * gain_two, unit_two, scale_two)
    resid_grad_all = group_gather(resid_grad.astype(BF16))
    home_out = grads_home(product_tokens(resid_grad_all, mixed, BF16))
    grad_mix = product(resid_grad_all, w_out, BF16)
    grad_q, *kv_grads = attend_back(info, q_low, grad_mix, kv_blocks, q_len)

    kv_total = kv_grads[-1]
    for s in range(seq_size - 2, -1, -1):
        got = lax.ppermute(kv_total, "seq", back)
        kv_total = got.astype(F32) + kv_grads[s].astype(F32)
        if s > 0:
            kv_total = kv_total.astype(BF16)
    kv_total = kv_total.astype(F32)

    def head_back(grad_rot, raw_vals, scale_vals, gain_vals):
        grad_unit = grad_rot * cos_t + turn_back(grad_rot * sin_t)
        unit_vals = raw_vals * scale_vals
        gain_grad = jnp.sum(grad_unit * unit_vals, axis=(0, 1, 2))
        return (rms_back(grad_unit * gain_vals, unit_vals, scale_vals), gain_grad)

    grad_q_raw, gain_q_part = head_back(grad_q.reshape(q_raw.shape), q_raw, q_scale, gain_q)
    grad_k_raw, gain_k_part = head_back(
        kv_total[:, :HD].reshape(k_raw.shape), k_raw, k_scale, gain_k
    )
    grad_qkv = jnp.concatenate(
        [grad_q_raw.reshape(-1, q_cols), grad_k_raw.reshape(-1, HD), kv_total[:, HD:]], axis=1
    ).astype(BF16)
    home_qkv = grads_home(product_tokens(act_one, grad_qkv, BF16))
    grad_act_one = group_scatter(product_wide(grad_qkv, w_qkv, BF16), q_len)
    gain_one_part = jnp.sum(grad_act_one * unit_one, axis=0)
    input_grad = resid_grad + rms_back(grad_act_one * gain_one, unit_one, scale_one)

    gain_parts = jnp.concatenate(
        [unmix(gain_one_part), unmix(gain_two_part), gain_q_part, gain_k_part]
    )
    grad_g = lax.psum_scatter(
        lax.psum(gain_parts, "tensor"), ("dp", "seq"), scatter_dimension=0, tiled=True
    )

    homes = (
        (home_qkv, 0),
        (home_qkv, q_cols),
        (home_qkv, q_cols + k_cols),
        (home_out, 0),
        (home_gu, 0),
        (home_gu, f_cols),
        (home_down, 0),
    )
    grad_w = jnp.concatenate(
        [home[d][:, at : at + w] for (home, at), w in zip(homes, widths) for d in range(dp_size)],
        axis=1,
    ).astype(F32)
    first_w, second_w, update_w = adam_part(master, grad_w, moment_m, moment_v)
    first_g, second_g, update_g = adam_part(gains, grad_g, gains_m, gains_v)
    gain_index = (dp_at * seq_size + seq_at) * gain_len + jnp.arange(gain_len, dtype=jnp.int32)
    edges = (0, D, 2 * D, 2 * D + HD, 2 * D + 2 * HD)
    member = [(gain_index >= a) & (gain_index < b) for a, b in zip(edges[:-1], edges[1:])]

    def square_sums(mat_vals, gain_vals):
        cols = jnp.sum(mat_vals * mat_vals, axis=0)
        mats = [jnp.sum(cols[a:b]) for a, b in zip(starts[:-1], starts[1:])]
        squares = gain_vals * gain_vals / tensor_size
        return mats + [jnp.sum(jnp.where(m, squares, 0.0)) for m in member]

    sums = jnp.stack(square_sums(master, gains) + square_sums(update_w, update_g))
    sums = lax.psum(sums, ("dp", "seq", "tensor"))
    weight_norm = jnp.sqrt(sums[:PARTS])
    update_norm = jnp.sqrt(sums[PARTS:])
    trust = weight_norm / (update_norm + ADAM_EPS)
    trust_w = jnp.concatenate(
        [jnp.broadcast_to(trust[m], (wide[m],)) for m in range(7)]
    )
    trust_g = sum(jnp.where(m, trust[7 + i], 0.0) for i, m in enumerate(member))
    new_w = master - LEARN_RATE * trust_w[None, :] * update_w
    new_g = gains - LEARN_RATE * trust_g * update_g

    def both(values):
        mine = unmix(values)
        other = swap_core(mine)
        first = core_at == 0
        return jnp.stack([jnp.where(first, mine, other), jnp.where(first, other, mine)])

    return (
        both(block_out.astype(BF16)),
        both(input_grad),
        new_w,
        first_w,
        second_w,
        new_w.astype(BF16),
        new_g,
        first_g,
        second_g,
        jnp.stack([weight_norm, update_norm]),
    )


def solution(mesh):
    in_specs = (
        P("dp", "seq", None),
        P("dp", "seq", None),
        P("dp"),
        P(("dp", "seq"), "tensor"),
        P(("dp", "seq"), "tensor"),
        P(("dp", "seq"), "tensor"),
        P(("dp", "seq")),
        P(("dp", "seq")),
        P(("dp", "seq")),
    )
    out_specs = (
        P("dp", "seq", None),
        P("dp", "seq", None),
        P(("dp", "seq"), "tensor"),
        P(("dp", "seq"), "tensor"),
        P(("dp", "seq"), "tensor"),
        P(("dp", "seq"), "tensor"),
        P(("dp", "seq")),
        P(("dp", "seq")),
        P(("dp", "seq")),
        P(),
    )
    return jax.shard_map(
        per_device, mesh=mesh, in_specs=in_specs, out_specs=out_specs, check_vma=False
    )
```
